32 devices in a mesh: row: 8 (over z, y), col: 4 (over x, core).
Axes of the slice: x: 2, y: 2, z: 4, core: 2. Of those that a mesh axis runs over, the one named last changes fastest.
Arguments:
- valence: bfloat16 [32768, 2048], P('row', 'col')
- conduction: bfloat16 [32768, 1024], P('row', 'col')
- point_index: int32 [8192], replicated, may hold values from 0 to 32767, as said below
Outputs:
- gram: float32 [8192, 8192], P('col', 'row')
The draws below stay inside these ranges and needn't reach their ends.
Inputs may be any that keep to these rules, and one draw needn't show every extreme that they name: `point_index`: 8192 distinct cells; cell g lies in slab g // 4096. In each aligned block of 1024 entries, at most 256 lie in any one slab, and in every block some slab holds exactly 256.
All inputs are finite; a program needn't handle non-finite values.
Results may differ from the reference program's by a relative error of at most 0.0003.
Values may be sent and summed in bfloat16 or wider, within the bound.
A program may use at most 128 MiB of HBM per device.

```python
import jax
import jax.numpy as jnp
from jax import lax

NV = 2048
NC = 1024
NP = 8192
GRID_DEV = 4096
PR = 1024
CAP = 256
N_ROW = 8


mode_count = 16


def orbital_draw(key, rows, bands):
    noise_key, coef_key, mode_key = jax.random.split(key, 3)
    noise = jax.random.normal(noise_key, (rows, bands), jnp.float32)
    coefs = 0.5 * jax.random.normal(coef_key, (rows, mode_count), jnp.float32)
    modes = jax.random.normal(mode_key, (mode_count, bands), jnp.float32)
    values = (noise + jnp.dot(coefs, modes)) / jnp.sqrt(5.0 * bands)
    return values.astype(jnp.bfloat16)


def draw_valence(key, part):
    return orbital_draw(key, GRID_DEV * N_ROW, NV)


def draw_conduction(key, part):
    return orbital_draw(jax.random.fold_in(key, 11), GRID_DEV * N_ROW, NC)


def draw_point_index(key, part):
    slots = N_ROW * CAP
    score_key, favor_key, cell_key, order_key = jax.random.split(key, 4)
    scores = jax.random.randint(score_key, (N_ROW, slots), 0, 1 << 16) * slots
    scores = scores + jnp.arange(slots, dtype=jnp.int32)[None, :]
    favored = jax.random.randint(favor_key, (N_ROW,), 0, N_ROW)
    slot_slab = jnp.arange(slots, dtype=jnp.int32) // CAP
    scores = scores + jnp.where(slot_slab[None, :] == favored[:, None], 1 << 29, 0)
    chosen = lax.top_k(scores, PR)[1].astype(jnp.int32)
    slab = chosen // CAP
    within = chosen - slab * CAP
    perms = jax.vmap(lambda k: jax.random.permutation(k, GRID_DEV))(jax.random.split(cell_key, N_ROW)).astype(jnp.int32)
    block_ids = jnp.arange(N_ROW, dtype=jnp.int32)[:, None]
    local = perms[slab, block_ids * CAP + within]
    cells = slab * GRID_DEV + local
    orders = jax.vmap(lambda k: jax.random.permutation(k, PR))(jax.random.split(order_key, N_ROW)).astype(jnp.int32)
    cells = jnp.take_along_axis(cells, orders, axis=1)
    return cells.reshape(NP).astype(jnp.int32)


def setup_inputs(seed: int = 0) -> dict:
    key_of = jax.random.split(jax.random.key(seed), 4)
    return {
        "valence": draw_valence(jax.random.fold_in(key_of[3], 71), 0),
        "conduction": draw_conduction(jax.random.fold_in(key_of[3], 71), 0),
        "point_index": draw_point_index(jax.random.fold_in(key_of[3], 71), 0),
    }


def full_total(rows, cols):
    left = rows.astype(jnp.float32)
    right = cols.astype(jnp.float32)
    return jnp.dot(left, right.T, precision=lax.Precision.HIGHEST)


def reference(valence, conduction, point_index):
    psi_mu = jnp.take(valence, point_index, axis=0)
    phi_mu = jnp.take(conduction, point_index, axis=0)
    psi_blocks = psi_mu.reshape(NP // PR, PR, NV)
    phi_blocks = phi_mu.reshape(NP // PR, PR, NC)

    def one_block(pair):
        return full_total(pair[0], psi_mu) * full_total(pair[1], phi_mu)

    stacked = lax.map(one_block, (psi_blocks, phi_blocks))
    return stacked.reshape(NP, NP)
```

```python
import functools
import math

import jax
import jax.numpy as jnp
from jax import lax
from jax.experimental import pallas as pl
from jax.experimental.pallas import tpu as pltpu
from jax.sharding import PartitionSpec as P

MESH = pl.DeviceIdType.MESH
UNIT_ROWS = 256
TILE = 256
LEAD = 2


def gram_kernel(
    n, c, cap, kv, splits,
    xv_ref, xc_ref, slot_ref, o_ref,
    got, pick, full, own, cond,
    trade_send, trade_recv, up_send, down_send, pair_send, piece_recv, own_send, own_recv,
):
    chunks, _, g = got.shape
    points = slot_ref.shape[0]
    span = n // c
    pairs = c // 2
    m = n // 2
    rows_unit = points // splits
    units = chunks * splits
    share = n // splits
    row, col = lax.axis_index("row"), lax.axis_index("col")
    z, y = row // 2, lax.rem(row, 2)
    pair = row + 1 - 2 * y
    core, chip = lax.rem(col, 2), col // 2
    mate = chip * 2 + 1 - core
    home, home_s = row // span, lax.rem(row, span)
    home_core = lax.rem(home, 2)
    is_root = col == home
    is_peer = (core == home_core) & (col != home)
    is_far = core != home_core

    def part_of(j):
        t = lax.rem(j - 2 * col + 2 * n, n)
        return t // c, lax.rem(t, c)

    my_shard = part_of(row)[1]
    keeps = (my_shard == col).astype(jnp.int32)

    def trade_target(i):
        e = lax.rem(i + row, n)
        s, cd = e // c, lax.rem(e, c)
        return lax.rem(s * c + col + 2 * cd, n), cd, s

    barrier = pltpu.get_barrier_semaphore()

    def greet(r, k):
        pl.semaphore_signal(barrier, inc=1, device_id=(r, k), device_id_type=MESH)

    def greet_trade(i, _):
        target, cd, _ = trade_target(i)

        @pl.when((target != row) | (cd != col))
        def _():
            greet(target, cd)

        @pl.when((i != row) | (my_shard != col))
        def _():
            greet(i, my_shard)

        return 0

    lax.fori_loop(0, n, greet_trade, 0)

    @pl.when(z > 0)
    def _():
        greet(row - 2, col)

    @pl.when(z + 1 < m)
    def _():
        greet(row + 2, col)

    greet(pair, col)
    greet(row, mate)
    for p in range(1, pairs):
        greet(row, lax.rem(chip + p, pairs) * 2 + core)
    ends = (z > 0).astype(jnp.int32) + (z + 1 < m).astype(jnp.int32)
    pl.semaphore_wait(barrier, 2 * (n - keeps) + ends + 2 + pairs - 1)

    def trade(k, i):
        target, cd, s = trade_target(i)
        rows = pl.ds(pl.multiple_of((cd * span + s) * cap, cap), cap)
        dst = got.at[k, pl.ds(pl.multiple_of(row * cap, cap), cap)]

        def ship(src):
            stays = (target == row) & (cd == col)

            @pl.when(stays)
            def _():
                pltpu.make_async_copy(src, dst, trade_recv.at[k]).start()

            @pl.when(jnp.logical_not(stays))
            def _():
                pltpu.make_async_remote_copy(
                    src_ref=src, dst_ref=dst,
                    send_sem=trade_send.at[k], recv_sem=trade_recv.at[k],
                    device_id=(target, cd), device_id_type=MESH,
                ).start()

        @pl.when(k < kv)
        def _():
            ship(xv_ref.at[rows, pl.ds(pl.multiple_of(k * g, g), g)])

        @pl.when(k >= kv)
        def _():
            ship(xc_ref.at[rows, pl.ds(pl.multiple_of((k - kv) * g, g), g)])

    def trade_portion(p):
        k, first = p // splits, lax.rem(p, splits) * share

        def one(i, _):
            trade(k, first + i)
            return 0

        lax.fori_loop(0, share, one, 0)

    def opening(p, _):
        trade_portion(p)
        return 0

    lead = splits + min(LEAD, splits)
    lax.fori_loop(0, lead, opening, 0)

    lanes = 128

    def build_pick(a, _):
        first = pl.multiple_of(a * lanes, lanes)
        place = lax.broadcasted_iota(jnp.int32, (points, lanes), 1) + first
        chosen = slot_ref[...] == place
        pick[:, pl.ds(first, lanes)] = jnp.where(chosen, 1.0, 0.0).astype(jnp.bfloat16)
        return 0

    lax.fori_loop(0, n * cap // lanes, build_pick, 0)

    block = 128

    def clear(a, _):
        rows = pl.ds(pl.multiple_of(a * block, block), block)
        o_ref[rows, :] = jnp.zeros((block, points), jnp.float32)
        cond[rows, :] = jnp.zeros((block, points), jnp.float32)
        return 0

    lax.fori_loop(0, span * points // block, clear, 0)

    def unit_rows(u):
        return u // splits, pl.ds(pl.multiple_of(lax.rem(u, splits) * rows_unit, rows_unit), rows_unit)

    def unit(j, u):
        k, rows = unit_rows(u)
        return full.at[j, k, rows]

    def send(j, u, sems, target_row):
        ref = unit(j, u)
        return pltpu.make_async_remote_copy(
            src_ref=ref, dst_ref=ref,
            send_sem=sems.at[j], recv_sem=piece_recv.at[j, u],
            device_id=(target_row, col), device_id_type=MESH,
        )

    def own_copy(q, u, src, slot, target_col):
        k, rows = unit_rows(u)
        return pltpu.make_async_remote_copy(
            src_ref=src, dst_ref=own.at[q, k, rows],
            send_sem=own_send.at[slot], recv_sem=own_recv.at[q, u],
            device_id=(row, target_col), device_id_type=MESH,
        )

    def own_unit(q, u):
        k, rows = unit_rows(u)
        return own.at[q, k, rows]

    def go_up(j, u):
        @pl.when(z + 1 < m)
        def _():
            send(j, u, up_send, row + 2).start()

    def go_down(j, u):
        @pl.when(z > 0)
        def _():
            send(j, u, down_send, row - 2).start()

    def go_pair(j, u):
        send(j, u, pair_send, pair).start()

    def spread_own(j, u):
        s, q = part_of(j)

        @pl.when(is_root & (s == home_s))
        def _():
            for p in range(1, pairs):
                own_copy(q, u, unit(j, u), p, lax.rem(chip + p, pairs) * 2 + core).start()
            own_copy(q, u, unit(j, u), 0, mate).start()

    def arrived(j, u):
        send(j, u, pair_send, pair).wait_recv()

    def compact(v):
        k, rows = unit_rows(v)

        @pl.when(lax.rem(v, splits) == 0)
        def _():
            pltpu.make_async_copy(got.at[k], got.at[k], trade_recv.at[k]).wait()

        dense = lax.dot_general(
            pick[rows, :], got[k], (((1,), (0,)), ((), ())), preferred_element_type=jnp.float32
        )
        full[row, k, rows, :] = dense.astype(jnp.bfloat16)

    def multiply(k, i):
        s, q = i // c, lax.rem(i, c)
        j = lax.rem(i + 2 * col, n)
        rows = pl.ds(pl.multiple_of(s * points, points), points)

        def tile(a, _):
            cols = pl.ds(pl.multiple_of(a * min(TILE, points), min(TILE, points)), min(TILE, points))
            part = lax.dot_general(
                full[j, k], own[q, k, cols, :], (((1,), (1,)), ((), ())),
                preferred_element_type=jnp.float32,
            )

            @pl.when(k < kv)
            def _():
                o_ref[rows, cols] += part

            @pl.when(k >= kv)
            def _():
                cond[rows, cols] += part

            return 0

        lax.fori_loop(0, points // min(TILE, points), tile, 0)

    compact(0)
    settle = m + 2 + splits - 1

    def step(t, _):
        @pl.when(t + lead < units)
        def _():
            trade_portion(t + lead)

        @pl.when(t < units)
        def _():
            go_up(row, t)
            go_down(row, t)
            go_pair(row, t)
            spread_own(row, t)

        def along(d, _):
            u = t - d

            @pl.when((u >= 0) & (u < units))
            def _():
                @pl.when(z >= d)
                def _():
                    j = row - 2 * d
                    arrived(j, u)
                    go_up(j, u)
                    go_pair(j, u)
                    spread_own(j, u)

                @pl.when(z + d < m)
                def _():
                    j = row + 2 * d
                    arrived(j, u)
                    go_down(j, u)
                    go_pair(j, u)
                    spread_own(j, u)

            return 0

        lax.fori_loop(1, m, along, 0)

        @pl.when(t + 1 < units)
        def _():
            compact(t + 1)

        def across(a, _):
            u = t - 1 - jnp.abs(a - z)

            @pl.when((u >= 0) & (u < units))
            def _():
                j = 2 * a + 1 - y
                arrived(j, u)
                spread_own(j, u)

            return 0

        lax.fori_loop(0, m, across, 0)

        def take_peer(q, _):
            u = t - m - 1

            @pl.when(is_peer & (u >= 0) & (u < units))
            def _():
                copy = own_copy(q, u, own_unit(q, u), 0, mate)
                copy.wait_recv()
                copy.start()

            return 0

        lax.fori_loop(0, c, take_peer, 0)

        def take_far(q, _):
            u = t - m - 2

            @pl.when(is_far & (u >= 0) & (u < units))
            def _():
                own_copy(q, u, own_unit(q, u), 0, mate).wait_recv()

            return 0

        lax.fori_loop(0, c, take_far, 0)

        w = t - settle

        @pl.when((w >= 0) & (w < units))
        def _():
            k, r = w // splits, lax.rem(w, splits)

            @pl.when(is_root & (r == 0))
            def _():
                def keep(q, _):
                    own[q, k] = full[lax.rem(home_s * c + q + 2 * col, n), k]
                    return 0

                lax.fori_loop(0, c, keep, 0)

            def some(i, _):
                multiply(k, r * share + i)
                return 0

            lax.fori_loop(0, share, some, 0)

        return 0

    lax.fori_loop(0, units + settle, step, 0)

    def finish(a, _):
        rows = pl.ds(pl.multiple_of(a * block, block), block)
        o_ref[rows, :] = o_ref[rows, :] * cond[rows, :]
        return 0

    lax.fori_loop(0, span * points // block, finish, 0)

    def drain(d, _):
        def piece_done(sems, j):
            pltpu.make_async_copy(full.at[0], full.at[0], sems.at[j]).wait()

        @pl.when(z >= d)
        def _():
            j = row - 2 * d

            @pl.when(z + 1 < m)
            def _():
                piece_done(up_send, j)

            piece_done(pair_send, j)

        @pl.when(z + d < m)
        def _():
            j = row + 2 * d

            @pl.when(z > 0)
            def _():
                piece_done(down_send, j)

            @pl.when(d > 0)
            def _():
                piece_done(pair_send, j)

        return 0

    lax.fori_loop(0, m, drain, 0)

    @pl.when(is_root)
    def _():
        for p in range(pairs):
            pltpu.make_async_copy(own, own, own_send.at[p]).wait()

    @pl.when(is_peer)
    def _():
        pltpu.make_async_copy(own, own, own_send.at[0]).wait()

    def drain_trade(k, _):
        @pl.when(keeps == 1)
        def _():
            rest = got.at[k, pl.ds(0, (n - 1) * cap)]
            pltpu.make_async_copy(rest, rest, trade_send.at[k]).wait()

        @pl.when(keeps == 0)
        def _():
            pltpu.make_async_copy(got.at[k], got.at[k], trade_send.at[k]).wait()

        return 0

    lax.fori_loop(0, chunks, drain_trade, 0)


def trade_spread_multiply(xv, xc, slots, n, c, cap):
    points = slots.shape[0]
    wv, wc = xv.shape[1], xc.shape[1]
    span = n // c
    pairs = c // 2
    g = math.gcd(wv, wc)
    chunks = (wv + wc) // g
    splits = max(points // UNIT_ROWS, 1)
    units = chunks * splits
    dma = pltpu.SemaphoreType.DMA
    return pl.pallas_call(
        functools.partial(gram_kernel, n, c, cap, wv // g, splits),
        out_shape=pltpu.VMEM((span * points, points), jnp.float32),
        in_specs=[
            pl.BlockSpec(memory_space=pl.ANY),
            pl.BlockSpec(memory_space=pl.ANY),
            pl.BlockSpec(memory_space=pltpu.VMEM),
        ],
        out_specs=pl.BlockSpec(memory_space=pltpu.VMEM),
        scratch_shapes=[
            pltpu.VMEM((chunks, n * cap, g), jnp.bfloat16),
            pltpu.VMEM((points, n * cap), jnp.bfloat16),
            pltpu.VMEM((n, chunks, points, g), jnp.bfloat16),
            pltpu.VMEM((c, chunks, points, g), jnp.bfloat16),
            pltpu.VMEM((span * points, points), jnp.float32),
            dma((chunks,)),
            dma((chunks,)),
            dma((n,)),
            dma((n,)),
            dma((n,)),
            dma((n, units)),
            dma((pairs,)),
            dma((c, units)),
        ],
        compiler_params=pltpu.CompilerParams(
            collective_id=0, has_side_effects=True, vmem_limit_bytes=50 * 1024 * 1024
        ),
    )(xv, xc, slots)


def on_device(valence, conduction, point_index):
    n = lax.axis_size("row")
    c = lax.axis_size("col")
    row, col = lax.axis_index("row"), lax.axis_index("col")
    grid_cells = valence.shape[0]
    points = point_index.shape[0] // n
    cap = max(2 * points // n, 2)
    blocks = point_index.reshape(n, points)
    owners = blocks // grid_cells
    offsets = blocks - owners * grid_cells
    onehot = owners[:, None, :] == jnp.arange(n, dtype=jnp.int32)[None, :, None]
    place = jnp.arange(points, dtype=jnp.int32)
    earlier = (place[:, None] < place[None, :]).astype(jnp.bfloat16)
    before = lax.dot_general(
        onehot.astype(jnp.bfloat16), earlier, (((2,), (0,)), ((), ())),
        preferred_element_type=jnp.float32,
    )
    ranks = jnp.sum(jnp.where(onehot, before, 0.0), axis=1).astype(jnp.int32)
    picked = (owners == row)[:, None, :] & (
        ranks[:, None, :] == jnp.arange(cap, dtype=jnp.int32)[None, :, None]
    )
    source_cells = jnp.sum(jnp.where(picked, offsets[:, None, :], 0), axis=2).reshape(n * cap)
    piece = lax.rem(row - 2 * col + 2 * n, n) // c + col * (n // c)
    slots = lax.dynamic_index_in_dim(owners * cap + ranks, piece, 0, keepdims=False)
    slots = jnp.broadcast_to(slots[:, None], (points, 128))
    xv = valence.at[source_cells].get(mode="promise_in_bounds")
    xc = conduction.at[source_cells].get(mode="promise_in_bounds")
    return trade_spread_multiply(xv, xc, slots, n, c, cap)


def solution(mesh):
    placed = (P("row", "col"), P("row", "col"), P())
    return jax.shard_map(
        on_device, mesh=mesh, in_specs=placed, out_specs=P("col", "row"), check_vma=False
    )
```

```python
import functools

import jax
import jax.numpy as jnp
from jax import lax
from jax.experimental import pallas as pl
from jax.experimental.pallas import tpu as pltpu
from jax.sharding import PartitionSpec as P

MESH = pl.DeviceIdType.MESH
UNIT_ROWS = 128
TILE = 256
LEAD = 1
HOP = 1
BAND = 1024


def gram_kernel(
    n, c, cap, kv, splits,
    val_ref, con_ref, cell_ref, slot_ref, o_ref,
    stage, wide, loose, packed, got, pick, full, own,
    load_sem, trade_send, trade_recv, up_send, down_send, pair_send, piece_recv, own_send, own_recv,
):
    chunks, _, g = got.shape
    points = slot_ref.shape[0]
    span = n // c
    pairs = c // 2
    m = n // 2
    block = 128
    rows_unit = points // splits
    units = chunks * splits
    share = n // splits
    row, col = lax.axis_index("row"), lax.axis_index("col")
    z, y = row // 2, lax.rem(row, 2)
    pair = row + 1 - 2 * y
    core, chip = lax.rem(col, 2), col // 2
    mate = chip * 2 + 1 - core
    home, home_s = row // span, lax.rem(row, span)
    home_core = lax.rem(home, 2)
    is_root = col == home
    is_peer = (core == home_core) & (col != home)
    is_far = core != home_core

    def part_of(p):
        t = lax.rem(p - 2 * col + 2 * n, n)
        return t // c, lax.rem(t, c)

    def place_of(s, q, k):
        return lax.rem(s * c + q + 2 * k, n)

    my_shard = part_of(row)[1]
    keeps = (my_shard == col).astype(jnp.int32)

    def trade_target(i):
        e = lax.rem(i + row, n)
        s, k = e // c, lax.rem(e, c)
        return place_of(s, col, k), k, s

    def load(k):
        src = val_ref if k < kv else con_ref
        first = (k if k < kv else k - kv) * g
        return pltpu.make_async_copy(src.at[:, pl.ds(first, g)], stage.at[k], load_sem.at[k])

    for k in range(chunks):
        load(k).start()

    barrier = pltpu.get_barrier_semaphore()

    def greet(r, k):
        pl.semaphore_signal(barrier, inc=1, device_id=(r, k), device_id_type=MESH)

    def greet_trade(i, _):
        target, k, _ = trade_target(i)

        @pl.when((target != row) | (k != col))
        def _():
            greet(target, k)

        @pl.when((i != row) | (my_shard != col))
        def _():
            greet(i, my_shard)

        return 0

    lax.fori_loop(0, n, greet_trade, 0)

    @pl.when(z > 0)
    def _():
        greet(row - 2, col)

    @pl.when(z + 1 < m)
    def _():
        greet(row + 2, col)

    greet(pair, col)
    greet(row, mate)
    for p in range(1, pairs):
        greet(row, lax.rem(chip + p, pairs) * 2 + core)
    ends = (z > 0).astype(jnp.int32) + (z + 1 < m).astype(jnp.int32)
    pl.semaphore_wait(barrier, 2 * (n - keeps) + ends + 2 + pairs - 1)

    messages = chunks * n
    cells = wide.shape[0]

    def message_rows(j):
        target, cd, s = trade_target(lax.rem(j, n))
        first = pl.multiple_of((cd * span + s) * cap, cap)
        return target, cd, j // n, first

    def widen(k):
        for a in range(chunks):
            @pl.when(k == a)
            def _():
                load(a).wait()

        def some(b, _):
            rows = pl.ds(pl.multiple_of(b * block, block), block)
            wide[rows, :] = stage[k, rows, :].astype(jnp.float32)
            return 0

        lax.fori_loop(0, cells // block, some, 0)

    def collect(j):
        _, _, k, first = message_rows(j)

        @pl.when(lax.rem(j, n) == 0)
        def _():
            widen(k)

        def some(a, _):
            base = pl.multiple_of(a * 16, 16)
            for r in range(16):
                cell = cell_ref[first + base + r]
                loose[pl.ds(base + r, 1), :] = wide[pl.ds(cell, 1), :]
            return 0

        lax.fori_loop(0, cap // 16, some, 0)
        packed[k, pl.ds(first, cap), :] = loose[...].astype(jnp.bfloat16)

    def ship(j):
        target, cd, k, first = message_rows(j)
        mine = pl.ds(pl.multiple_of(row * cap, cap), cap)
        stays = (target == row) & (cd == col)

        @pl.when(stays)
        def _():
            got[k, mine, :] = packed[k, pl.ds(first, cap), :]

        @pl.when(jnp.logical_not(stays))
        def _():
            pltpu.make_async_remote_copy(
                src_ref=packed.at[k, pl.ds(first, cap)], dst_ref=got.at[k, mine],
                send_sem=trade_send.at[k], recv_sem=trade_recv.at[k],
                device_id=(target, cd), device_id_type=MESH,
            ).start()

    def trade_portion(p):
        def one(i, _):
            j = p * share + i
            collect(j)

            @pl.when(j > 0)
            def _():
                ship(j - 1)

            return 0

        lax.fori_loop(0, share, one, 0)

    def opening(p, _):
        trade_portion(p)
        return 0

    lead = splits + min(LEAD, splits)
    lax.fori_loop(0, lead, opening, 0)

    lanes = 128

    def build_pick(a, _):
        first = pl.multiple_of(a * lanes, lanes)
        place = lax.broadcasted_iota(jnp.int32, (points, lanes), 1) + first
        chosen = slot_ref[...] == place
        pick[:, pl.ds(first, lanes)] = jnp.where(chosen, 1.0, 0.0).astype(jnp.bfloat16)
        return 0

    lax.fori_loop(0, n * cap // lanes, build_pick, 0)

    def unit_rows(u):
        return u // splits, pl.ds(pl.multiple_of(lax.rem(u, splits) * rows_unit, rows_unit), rows_unit)

    def unit(p, u):
        k, rows = unit_rows(u)
        return full.at[p, k, rows]

    def send(p, u, sems, target_row):
        ref = unit(p, u)
        return pltpu.make_async_remote_copy(
            src_ref=ref, dst_ref=ref,
            send_sem=sems.at[p], recv_sem=piece_recv.at[p, u],
            device_id=(target_row, col), device_id_type=MESH,
        )

    def own_copy(q, u, src, slot, target_col):
        k, rows = unit_rows(u)
        return pltpu.make_async_remote_copy(
            src_ref=src, dst_ref=own.at[q, k, rows],
            send_sem=own_send.at[slot], recv_sem=own_recv.at[q, u],
            device_id=(row, target_col), device_id_type=MESH,
        )

    def own_unit(q, u):
        k, rows = unit_rows(u)
        return own.at[q, k, rows]

    def route(p):
        oz, same = p // 2, lax.rem(p, 2) == y
        up = same & (z >= oz) & (z + 1 < m)
        down = same & (z <= oz) & (z > 0)
        hops = jnp.abs(z - oz) + jnp.where(same, 0, 1)
        return up, down, same, hops

    def spread(p, u):
        up, down, cross, _ = route(p)

        @pl.when(up)
        def _():
            send(p, u, up_send, row + 2).start()

        @pl.when(down)
        def _():
            send(p, u, down_send, row - 2).start()

        @pl.when(cross)
        def _():
            send(p, u, pair_send, pair).start()

        s, q = part_of(p)

        @pl.when(is_root & (s == home_s))
        def _():
            for a in range(1, pairs):
                own_copy(q, u, unit(p, u), a, lax.rem(chip + a, pairs) * 2 + core).start()
            own_copy(q, u, unit(p, u), 0, mate).start()

    def trade_done(sems, k):
        for kept in range(2):
            @pl.when(keeps == kept)
            def _():
                part = got.at[k, pl.ds(0, (n - kept) * cap)]
                pltpu.make_async_copy(part, part, sems.at[k]).wait()

    def compact(v):
        k, rows = unit_rows(v)

        @pl.when(lax.rem(v, splits) == 0)
        def _():
            trade_done(trade_recv, k)

        dense = lax.dot_general(
            pick[rows, :], got[k], (((1,), (0,)), ((), ())), preferred_element_type=jnp.float32
        )
        full[row, k, rows, :] = dense.astype(jnp.bfloat16)

    tile = min(TILE, points)
    band = min(BAND, points)
    items = span * (points // tile)

    def multiply(k, i):
        s, a = i // (points // tile), lax.rem(i, points // tile)
        cols = pl.ds(pl.multiple_of(a * tile, tile), tile)

        def strip(b, _):
            inner = pl.ds(pl.multiple_of(b * band, band), band)
            rows = pl.ds(pl.multiple_of(s * points + b * band, band), band)
            total = None
            for q in range(c):
                part = lax.dot_general(
                    full[place_of(s, q, col), k, inner, :], own[q, k, cols, :],
                    (((1,), (1,)), ((), ())), preferred_element_type=jnp.float32,
                )
                total = part if total is None else total + part

            @pl.when(k == 0)
            def _():
                o_ref[rows, cols] = total

            @pl.when((k > 0) & (k < kv))
            def _():
                o_ref[rows, cols] += total

            @pl.when(k == kv)
            def _():
                o_ref[rows, cols] *= total

            return 0

        lax.fori_loop(0, points // band, strip, 0)

    compact(0)
    settle = HOP * (m + 2) + splits - 1

    def step(t, _):
        @pl.when(t + lead < units)
        def _():
            trade_portion(t + lead)

        @pl.when(t + lead == units)
        def _():
            ship(messages - 1)

        @pl.when(t < units)
        def _():
            spread(row, t)

        def pieces(p, _):
            hops = route(p)[3]
            u = t - HOP * hops

            @pl.when((hops > 0) & (u >= 0) & (u < units))
            def _():
                send(p, u, pair_send, pair).wait_recv()
                spread(p, u)

            return 0

        @pl.when(t + 1 < units)
        def _():
            compact(t + 1)

        lax.fori_loop(0, n, pieces, 0)

        def take_peer(q, _):
            u = t - HOP * (m + 1)

            @pl.when(is_peer & (u >= 0) & (u < units))
            def _():
                copy = own_copy(q, u, own_unit(q, u), 0, mate)
                copy.wait_recv()
                copy.start()

            return 0

        lax.fori_loop(0, c, take_peer, 0)

        def take_far(q, _):
            u = t - HOP * (m + 2)

            @pl.when(is_far & (u >= 0) & (u < units))
            def _():
                own_copy(q, u, own_unit(q, u), 0, mate).wait_recv()

            return 0

        lax.fori_loop(0, c, take_far, 0)

        w = t - settle

        @pl.when((w >= 0) & (w < units))
        def _():
            k, r = w // splits, lax.rem(w, splits)

            @pl.when(is_root & (r == 0))
            def _():
                def keep(q, _):
                    own[q, k] = full[place_of(home_s, q, col), k]
                    return 0

                lax.fori_loop(0, c, keep, 0)

            def some(i, _):
                multiply(k, r * (items // splits) + i)
                return 0

            lax.fori_loop(0, items // splits, some, 0)

        return 0

    lax.fori_loop(0, units + settle, step, 0)

    def drain(p, _):
        up, down, cross, _ = route(p)

        def piece_done(sems):
            pltpu.make_async_copy(full.at[0], full.at[0], sems.at[p]).wait()

        for goes, sems in ((up, up_send), (down, down_send), (cross, pair_send)):
            @pl.when(goes)
            def _():
                piece_done(sems)

        return 0

    lax.fori_loop(0, n, drain, 0)

    @pl.when(is_root)
    def _():
        for p in range(pairs):
            pltpu.make_async_copy(own, own, own_send.at[p]).wait()

    @pl.when(is_peer)
    def _():
        pltpu.make_async_copy(own, own, own_send.at[0]).wait()

    def drain_trade(k, _):
        trade_done(trade_send, k)
        return 0

    lax.fori_loop(0, chunks, drain_trade, 0)


def trade_spread_multiply(valence, conduction, source, slots, n, c, cap):
    points = slots.shape[0]
    wv, wc = valence.shape[1], conduction.shape[1]
    cells = valence.shape[0]
    span = n // c
    pairs = c // 2
    g = wc
    chunks = (wv + wc) // g
    splits = max(points // UNIT_ROWS, 1)
    units = chunks * splits
    dma = pltpu.SemaphoreType.DMA
    return pl.pallas_call(
        functools.partial(gram_kernel, n, c, cap, wv // g, splits),
        out_shape=pltpu.VMEM((span * points, points), jnp.float32),
        in_specs=[
            pl.BlockSpec(memory_space=pl.ANY),
            pl.BlockSpec(memory_space=pl.ANY),
            pl.BlockSpec(memory_space=pltpu.SMEM),
            pl.BlockSpec(memory_space=pltpu.VMEM),
        ],
        out_specs=pl.BlockSpec(memory_space=pltpu.VMEM),
        scratch_shapes=[
            pltpu.VMEM((chunks, cells, g), jnp.bfloat16),
            pltpu.VMEM((cells, g), jnp.float32),
            pltpu.VMEM((cap, g), jnp.float32),
            pltpu.VMEM((chunks, n * cap, g), jnp.bfloat16),
            pltpu.VMEM((chunks, n * cap, g), jnp.bfloat16),
            pltpu.VMEM((points, n * cap), jnp.bfloat16),
            pltpu.VMEM((n, chunks, points, g), jnp.bfloat16),
            pltpu.VMEM((c, chunks, points, g), jnp.bfloat16),
            dma((chunks,)),
            dma((chunks,)),
            dma((chunks,)),
            dma((n,)),
            dma((n,)),
            dma((n,)),
            dma((n, units)),
            dma((pairs,)),
            dma((c, units)),
        ],
        compiler_params=pltpu.CompilerParams(
            collective_id=0, has_side_effects=True, vmem_limit_bytes=50 * 1024 * 1024
        ),
    )(valence, conduction, source, slots)


def on_device(valence, conduction, point_index):
    n = lax.axis_size("row")
    c = lax.axis_size("col")
    row, col = lax.axis_index("row"), lax.axis_index("col")
    grid_cells = valence.shape[0]
    points = point_index.shape[0] // n
    cap = max(2 * points // n, 2)
    blocks = point_index.reshape(n, points)
    owners = blocks // grid_cells
    offsets = blocks - owners * grid_cells
    onehot = owners[:, None, :] == jnp.arange(n, dtype=jnp.int32)[None, :, None]
    place = jnp.arange(points, dtype=jnp.int32)
    earlier = (place[:, None] < place[None, :]).astype(jnp.bfloat16)
    before = lax.dot_general(
        onehot.astype(jnp.bfloat16), earlier, (((2,), (0,)), ((), ())),
        preferred_element_type=jnp.float32,
    )
    ranks = jnp.sum(jnp.where(onehot, before, 0.0), axis=1).astype(jnp.int32)
    picked = (owners == row)[:, None, :] & (
        ranks[:, None, :] == jnp.arange(cap, dtype=jnp.int32)[None, :, None]
    )
    source_cells = jnp.sum(jnp.where(picked, offsets[:, None, :], 0), axis=2).reshape(n * cap)
    piece = lax.rem(row - 2 * col + 2 * n, n) // c + col * (n // c)
    slots = lax.dynamic_index_in_dim(owners * cap + ranks, piece, 0, keepdims=False)
    slots = jnp.broadcast_to(slots[:, None], (points, 128))
    return trade_spread_multiply(valence, conduction, source_cells, slots, n, c, cap)


def solution(mesh):
    placed = (P("row", "col"), P("row", "col"), P())
    return jax.shard_map(
        on_device, mesh=mesh, in_specs=placed, out_specs=P("col", "row"), check_vma=False
    )
```

```python
import functools

import jax
import jax.numpy as jnp
from jax import lax
from jax.experimental import pallas as pl
from jax.experimental.pallas import tpu as pltpu
from jax.sharding import PartitionSpec as P

MESH = pl.DeviceIdType.MESH
UNIT_ROWS = 256
LANES = 128
FLAT = 4
TILE = 256
LEAD = 1
HOP = 1


def gram_kernel(
    n, c, cap, kv, splits, fold,
    val_ref, con_ref, cell_ref, slot_ref, o_ref,
    stage, wide, loose, packed, got, pick, full, own, cond,
    load_sem, trade_send, trade_recv, up_send, down_send, pair_send, piece_recv, own_send, own_recv,
):
    chunks, _, g = got.shape
    points = slot_ref.shape[0]
    span = n // c
    pairs = c // 2
    m = n // 2
    block = 128
    rows_unit = points // splits
    units = chunks * splits
    share = n // splits
    row, col = lax.axis_index("row"), lax.axis_index("col")
    z, y = row // 2, lax.rem(row, 2)
    pair = row + 1 - 2 * y
    core, chip = lax.rem(col, 2), col // 2
    mate = chip * 2 + 1 - core
    home, home_s = row // span, lax.rem(row, span)
    home_core = lax.rem(home, 2)
    is_root = col == home
    is_peer = (core == home_core) & (col != home)
    is_far = core != home_core

    def part_of(p):
        t = lax.rem(p - 2 * col + 2 * n, n)
        return t // c, lax.rem(t, c)

    def place_of(s, q, k):
        return lax.rem(s * c + q + 2 * k, n)

    my_shard = part_of(row)[1]
    keeps = (my_shard == col).astype(jnp.int32)

    def trade_target(i):
        e = lax.rem(i + row, n)
        s, k = e // c, lax.rem(e, c)
        return place_of(s, col, k), k, s

    def load(k):
        src = val_ref if k * fold < kv else con_ref
        first = (k * fold if k * fold < kv else k * fold - kv) * g
        return pltpu.make_async_copy(src.at[:, pl.ds(first, fold * g)], stage.at[k], load_sem.at[k])

    for k in range(chunks // fold):
        load(k).start()

    barrier = pltpu.get_barrier_semaphore()

    def greet(r, k):
        pl.semaphore_signal(barrier, inc=1, device_id=(r, k), device_id_type=MESH)

    def greet_trade(i, _):
        target, k, _ = trade_target(i)

        @pl.when((target != row) | (k != col))
        def _():
            greet(target, k)

        @pl.when((i != row) | (my_shard != col))
        def _():
            greet(i, my_shard)

        return 0

    lax.fori_loop(0, n, greet_trade, 0)

    @pl.when(z > 0)
    def _():
        greet(row - 2, col)

    @pl.when(z + 1 < m)
    def _():
        greet(row + 2, col)

    greet(pair, col)
    greet(row, mate)
    for p in range(1, pairs):
        greet(row, lax.rem(chip + p, pairs) * 2 + core)
    ends = (z > 0).astype(jnp.int32) + (z + 1 < m).astype(jnp.int32)
    pl.semaphore_wait(barrier, 2 * (n - keeps) + ends + 2 + pairs - 1)

    messages = chunks * n
    cells = wide.shape[0]

    def message_rows(j):
        target, cd, s = trade_target(lax.rem(j, n))
        first = pl.multiple_of((cd * span + s) * cap, cap)
        return target, cd, j // n, first

    def widen(k):
        for a in range(chunks // fold):
            @pl.when(k == a)
            def _():
                load(a).wait()

        def some(b, _):
            rows = pl.ds(pl.multiple_of(b * block, block), block)
            wide[rows, :] = stage[k, rows, :].astype(jnp.float32)
            return 0

        lax.fori_loop(0, cells // block, some, 0)

    def collect(j):
        _, _, k, first = message_rows(j)

        @pl.when(lax.rem(j, n * fold) == 0)
        def _():
            widen(k // fold)

        @pl.when(lax.rem(k, fold) == 0)
        def _():
            def some(a, _):
                base = pl.multiple_of(a * 16, 16)
                for r in range(16):
                    cell = cell_ref[first + base + r]
                    loose[pl.ds(base + r, 1), :] = wide[pl.ds(cell, 1), :]
                return 0

            lax.fori_loop(0, cap // 16, some, 0)
            for f in range(fold):
                packed[k + f, pl.ds(first, cap), :] = loose[:, f * g : (f + 1) * g].astype(jnp.bfloat16)

    def ship(j):
        target, cd, k, first = message_rows(j)
        mine = pl.ds(pl.multiple_of(row * cap, cap), cap)
        stays = (target == row) & (cd == col)

        @pl.when(stays)
        def _():
            got[k, mine, :] = packed[k, pl.ds(first, cap), :]

        @pl.when(jnp.logical_not(stays))
        def _():
            pltpu.make_async_remote_copy(
                src_ref=packed.at[k, pl.ds(first, cap)], dst_ref=got.at[k, mine],
                send_sem=trade_send.at[k], recv_sem=trade_recv.at[k],
                device_id=(target, cd), device_id_type=MESH,
            ).start()

    def trade_portion(p):
        def one(i, _):
            j = p * share + i
            collect(j)

            @pl.when(j > 0)
            def _():
                ship(j - 1)

            return 0

        lax.fori_loop(0, share, one, 0)

    def opening(p, _):
        trade_portion(p)
        return 0

    lead = splits + min(LEAD, splits)
    lax.fori_loop(0, lead, opening, 0)

    lanes = 128

    def build_pick(a, _):
        first = pl.multiple_of(a * lanes, lanes)
        place = lax.broadcasted_iota(jnp.int32, (points, lanes), 1) + first
        chosen = slot_ref[...] == place
        pick[:, pl.ds(first, lanes)] = jnp.where(chosen, 1.0, 0.0).astype(jnp.bfloat16)
        return 0

    lax.fori_loop(0, n * cap // lanes, build_pick, 0)

    def unit_rows(u):
        return u // splits, pl.ds(pl.multiple_of(lax.rem(u, splits) * rows_unit, rows_unit), rows_unit)

    def unit(p, u):
        k, rows = unit_rows(u)
        return full.at[p, k, rows]

    def send(p, u, sems, target_row):
        ref = unit(p, u)
        return pltpu.make_async_remote_copy(
            src_ref=ref, dst_ref=ref,
            send_sem=sems.at[p], recv_sem=piece_recv.at[p, u],
            device_id=(target_row, col), device_id_type=MESH,
        )

    def own_copy(q, u, src, slot, target_col):
        k, rows = unit_rows(u)
        return pltpu.make_async_remote_copy(
            src_ref=src, dst_ref=own.at[q, k, rows],
            send_sem=own_send.at[slot], recv_sem=own_recv.at[q, u],
            device_id=(row, target_col), device_id_type=MESH,
        )

    def own_unit(q, u):
        k, rows = unit_rows(u)
        return own.at[q, k, rows]

    def place(p):
        oz, same = p // 2, lax.rem(p, 2) == y
        rim = (oz == 0) | (oz == m - 1)
        rises = (z >= oz) & (z + 1 < m)
        falls = (z <= oz) & (z > 0)
        hops = jnp.abs(z - oz) + jnp.where(same, 0, 1)
        return same, rim, rises, falls, z == oz, hops

    def spread(p, u):
        same, rim, rises, falls, level, _ = place(p)
        flat = rim & (lax.rem(u, FLAT) == 0)

        @pl.when((same | flat) & rises)
        def _():
            send(p, u, up_send, row + 2).start()

        @pl.when((same | flat) & falls)
        def _():
            send(p, u, down_send, row - 2).start()

        @pl.when(same & (level | jnp.logical_not(flat)))
        def _():
            send(p, u, pair_send, pair).start()

        s, q = part_of(p)

        @pl.when(is_root & (s == home_s))
        def _():
            for a in range(1, pairs):
                own_copy(q, u, unit(p, u), a, lax.rem(chip + a, pairs) * 2 + core).start()
            own_copy(q, u, unit(p, u), 0, mate).start()

    def trade_done(sems, k):
        for kept in range(2):
            @pl.when(keeps == kept)
            def _():
                part = got.at[k, pl.ds(0, (n - kept) * cap)]
                pltpu.make_async_copy(part, part, sems.at[k]).wait()

    def compact(v):
        k, rows = unit_rows(v)

        @pl.when(lax.rem(v, splits) == 0)
        def _():
            trade_done(trade_recv, k)

        dense = lax.dot_general(
            pick[rows, :], got[k], (((1,), (0,)), ((), ())), preferred_element_type=jnp.float32
        )
        full[row, k, rows, :] = dense.astype(jnp.bfloat16)

    tile = min(TILE, points)
    items = span * (points // tile)

    def multiply(k, i):
        s, a = i // (points // tile), lax.rem(i, points // tile)
        cols = pl.ds(pl.multiple_of(a * tile, tile), tile)
        rows = pl.ds(pl.multiple_of(s * points, points), points)
        total = None
        for q in range(0, c, 2):
            left = jnp.concatenate([full[place_of(s, q + e, col), k] for e in range(2)], axis=1)
            right = jnp.concatenate([own[q + e, k, cols, :] for e in range(2)], axis=1)
            part = lax.dot_general(
                left, right, (((1,), (1,)), ((), ())), preferred_element_type=jnp.float32
            )
            total = part if total is None else total + part

        @pl.when(k == 0)
        def _():
            o_ref[rows, cols] = total

        @pl.when((k > 0) & (k < kv))
        def _():
            o_ref[rows, cols] += total

        @pl.when((k == kv) & (k < chunks - 1))
        def _():
            cond[rows, cols] = total

        @pl.when((k > kv) & (k < chunks - 1))
        def _():
            cond[rows, cols] += total

        @pl.when(k == chunks - 1)
        def _():
            whole = total if chunks - kv == 1 else cond[rows, cols] + total
            o_ref[rows, cols] *= whole

    compact(0)
    settle = HOP * (m + 2) + splits - 1

    def step(t, _):
        @pl.when(t + lead < units)
        def _():
            trade_portion(t + lead)

        @pl.when(t + lead == units)
        def _():
            ship(messages - 1)

        @pl.when(t < units)
        def _():
            spread(row, t)

        def pieces(p, _):
            hops = place(p)[5]
            u = t - HOP * hops

            @pl.when((hops > 0) & (u >= 0) & (u < units))
            def _():
                send(p, u, pair_send, pair).wait_recv()
                spread(p, u)

            return 0

        @pl.when(t + 1 < units)
        def _():
            compact(t + 1)

        lax.fori_loop(0, n, pieces, 0)

        def take_peer(q, _):
            u = t - HOP * (m + 1)

            @pl.when(is_peer & (u >= 0) & (u < units))
            def _():
                copy = own_copy(q, u, own_unit(q, u), 0, mate)
                copy.wait_recv()
                copy.start()

            return 0

        lax.fori_loop(0, c, take_peer, 0)

        def take_far(q, _):
            u = t - HOP * (m + 2)

            @pl.when(is_far & (u >= 0) & (u < units))
            def _():
                own_copy(q, u, own_unit(q, u), 0, mate).wait_recv()

            return 0

        lax.fori_loop(0, c, take_far, 0)

        w = t - settle

        @pl.when((w >= 0) & (w < units))
        def _():
            k, r = w // splits, lax.rem(w, splits)

            @pl.when(is_root & (r == 0))
            def _():
                def keep(q, _):
                    own[q, k] = full[place_of(home_s, q, col), k]
                    return 0

                lax.fori_loop(0, c, keep, 0)

            def some(i, _):
                multiply(k, r * (items // splits) + i)
                return 0

            lax.fori_loop(0, items // splits, some, 0)

        return 0

    lax.fori_loop(0, units + settle, step, 0)

    flats = (units + FLAT - 1) // FLAT

    def sent(sems, p, count):
        part = stage.at[0, pl.ds(0, count * rows_unit // fold)]
        pltpu.make_async_copy(part, part, sems.at[p]).wait()

    def drain(p, _):
        same, rim, rises, falls, level, _ = place(p)
        other = jnp.logical_not(same)
        short = rim & jnp.logical_not(level)
        for goes, sems, count in (
            (same & rises, up_send, units),
            (same & falls, down_send, units),
            (other & rim & rises, up_send, flats),
            (other & rim & falls, down_send, flats),
            (same & jnp.logical_not(short), pair_send, units),
            (same & short, pair_send, units - flats),
        ):
            @pl.when(goes)
            def _():
                sent(sems, p, count)

        return 0

    lax.fori_loop(0, n, drain, 0)

    @pl.when(is_root)
    def _():
        for p in range(pairs):
            pltpu.make_async_copy(own, own, own_send.at[p]).wait()

    @pl.when(is_peer)
    def _():
        pltpu.make_async_copy(own, own, own_send.at[0]).wait()

    def drain_trade(k, _):
        trade_done(trade_send, k)
        return 0

    lax.fori_loop(0, chunks, drain_trade, 0)


def trade_spread_multiply(valence, conduction, source, slots, n, c, cap):
    points = slots.shape[0]
    wv, wc = valence.shape[1], conduction.shape[1]
    cells = valence.shape[0]
    span = n // c
    pairs = c // 2
    g = LANES
    fold = 2 if wv % (2 * g) == 0 and wc % (2 * g) == 0 else 1
    chunks = (wv + wc) // g
    splits = max(points // UNIT_ROWS, 1)
    units = chunks * splits
    dma = pltpu.SemaphoreType.DMA
    return pl.pallas_call(
        functools.partial(gram_kernel, n, c, cap, wv // g, splits, fold),
        out_shape=pltpu.VMEM((span * points, points), jnp.float32),
        in_specs=[
            pl.BlockSpec(memory_space=pl.ANY),
            pl.BlockSpec(memory_space=pl.ANY),
            pl.BlockSpec(memory_space=pltpu.SMEM),
            pl.BlockSpec(memory_space=pltpu.VMEM),
        ],
        out_specs=pl.BlockSpec(memory_space=pltpu.VMEM),
        scratch_shapes=[
            pltpu.VMEM((chunks // fold, cells, fold * g), jnp.bfloat16),
            pltpu.VMEM((cells, fold * g), jnp.float32),
            pltpu.VMEM((cap, fold * g), jnp.float32),
            pltpu.VMEM((chunks, n * cap, g), jnp.bfloat16),
            pltpu.VMEM((chunks, n * cap, g), jnp.bfloat16),
            pltpu.VMEM((points, n * cap), jnp.bfloat16),
            pltpu.VMEM((n, chunks, points, g), jnp.bfloat16),
            pltpu.VMEM((c, chunks, points, g), jnp.bfloat16),
            pltpu.VMEM((span * points, points), jnp.float32),
            dma((chunks // fold,)),
            dma((chunks,)),
            dma((chunks,)),
            dma((n,)),
            dma((n,)),
            dma((n,)),
            dma((n, units)),
            dma((pairs,)),
            dma((c, units)),
        ],
        compiler_params=pltpu.CompilerParams(
            collective_id=0, has_side_effects=True, vmem_limit_bytes=50 * 1024 * 1024
        ),
    )(valence, conduction, source, slots)


def on_device(valence, conduction, point_index):
    n = lax.axis_size("row")
    c = lax.axis_size("col")
    row, col = lax.axis_index("row"), lax.axis_index("col")
    grid_cells = valence.shape[0]
    points = point_index.shape[0] // n
    cap = max(2 * points // n, 2)
    blocks = point_index.reshape(n, points)
    owners = blocks // grid_cells
    offsets = blocks - owners * grid_cells
    onehot = owners[:, None, :] == jnp.arange(n, dtype=jnp.int32)[None, :, None]
    place = jnp.arange(points, dtype=jnp.int32)
    earlier = (place[:, None] < place[None, :]).astype(jnp.bfloat16)
    before = lax.dot_general(
        onehot.astype(jnp.bfloat16), earlier, (((2,), (0,)), ((), ())),
        preferred_element_type=jnp.float32,
    )
    ranks = jnp.sum(jnp.where(onehot, before, 0.0), axis=1).astype(jnp.int32)
    picked = (owners == row)[:, None, :] & (
        ranks[:, None, :] == jnp.arange(cap, dtype=jnp.int32)[None, :, None]
    )
    source_cells = jnp.sum(jnp.where(picked, offsets[:, None, :], 0), axis=2).reshape(n * cap)
    piece = lax.rem(row - 2 * col + 2 * n, n) // c + col * (n // c)
    slots = lax.dynamic_index_in_dim(owners * cap + ranks, piece, 0, keepdims=False)
    slots = jnp.broadcast_to(slots[:, None], (points, 128))
    return trade_spread_multiply(valence, conduction, source_cells, slots, n, c, cap)


def solution(mesh):
    placed = (P("row", "col"), P("row", "col"), P())
    return jax.shard_map(
        on_device, mesh=mesh, in_specs=placed, out_specs=P("col", "row"), check_vma=False
    )
```

```python
import functools

import jax
import jax.numpy as jnp
from jax import lax
from jax.experimental import pallas as pl
from jax.experimental.pallas import tpu as pltpu
from jax.sharding import PartitionSpec as P

MESH = pl.DeviceIdType.MESH
UNIT_ROWS = 256
LANES = 128
FLAT = 4
TILE = 256
LEAD = 2
HOP = 1


def gram_kernel(
    n, c, cap, kv, splits, fold,
    val_ref, con_ref, cell_ref, slot_ref, o_ref,
    stage, wide, loose, packed, got, pick, full, own, cond,
    load_sem, trade_send, trade_recv, up_send, down_send, pair_send, piece_recv, own_send, own_recv,
):
    chunks, _, g = got.shape
    points = slot_ref.shape[0]
    span = n // c
    pairs = c // 2
    m = n // 2
    block = 128
    rows_unit = points // splits
    units = chunks * splits
    share = n // splits
    row, col = lax.axis_index("row"), lax.axis_index("col")
    z, y = row // 2, lax.rem(row, 2)
    pair = row + 1 - 2 * y
    core, chip = lax.rem(col, 2), col // 2
    mate = chip * 2 + 1 - core
    home, home_s = row // span, lax.rem(row, span)
    home_core = lax.rem(home, 2)
    is_root = col == home
    is_peer = (core == home_core) & (col != home)
    is_far = core != home_core

    def part_of(p):
        t = lax.rem(p - 2 * col + 2 * n, n)
        return t // c, lax.rem(t, c)

    def place_of(s, q, k):
        return lax.rem(s * c + q + 2 * k, n)

    my_shard = part_of(row)[1]
    keeps = (my_shard == col).astype(jnp.int32)

    def trade_target(i):
        e = lax.rem(i + row, n)
        s, k = e // c, lax.rem(e, c)
        return place_of(s, col, k), k, s

    def load(k):
        src = val_ref if k * fold < kv else con_ref
        first = (k * fold if k * fold < kv else k * fold - kv) * g
        return pltpu.make_async_copy(src.at[:, pl.ds(first, fold * g)], stage.at[k], load_sem.at[k])

    for k in range(chunks // fold):
        load(k).start()

    barrier = pltpu.get_barrier_semaphore()

    def greet(r, k):
        pl.semaphore_signal(barrier, inc=1, device_id=(r, k), device_id_type=MESH)

    def greet_trade(i, _):
        target, k, _ = trade_target(i)

        @pl.when((target != row) | (k != col))
        def _():
            greet(target, k)

        @pl.when((i != row) | (my_shard != col))
        def _():
            greet(i, my_shard)

        return 0

    lax.fori_loop(0, n, greet_trade, 0)

    @pl.when(z > 0)
    def _():
        greet(row - 2, col)

    @pl.when(z + 1 < m)
    def _():
        greet(row + 2, col)

    greet(pair, col)
    greet(row, mate)
    for p in range(1, pairs):
        greet(row, lax.rem(chip + p, pairs) * 2 + core)
    ends = (z > 0).astype(jnp.int32) + (z + 1 < m).astype(jnp.int32)
    pl.semaphore_wait(barrier, 2 * (n - keeps) + ends + 2 + pairs - 1)

    messages = chunks * n
    cells = wide.shape[0]

    def message_rows(j):
        target, cd, s = trade_target(lax.rem(j, n))
        first = pl.multiple_of((cd * span + s) * cap, cap)
        return target, cd, j // n, first

    def widen(k):
        for a in range(chunks // fold):
            @pl.when(k == a)
            def _():
                load(a).wait()

        def some(b, _):
            rows = pl.ds(pl.multiple_of(b * block, block), block)
            wide[rows, :] = stage[k, rows, :].astype(jnp.float32)
            return 0

        lax.fori_loop(0, cells // block, some, 0)

    def collect(j):
        _, _, k, first = message_rows(j)

        @pl.when(lax.rem(j, n * fold) == 0)
        def _():
            widen(k // fold)

        @pl.when(lax.rem(k, fold) == 0)
        def _():
            def some(a, _):
                base = pl.multiple_of(a * 16, 16)
                for r in range(16):
                    cell = cell_ref[first + base + r]
                    loose[pl.ds(base + r, 1), :] = wide[pl.ds(cell, 1), :]
                return 0

            lax.fori_loop(0, cap // 16, some, 0)
            for f in range(fold):
                packed[k + f, pl.ds(first, cap), :] = loose[:, f * g : (f + 1) * g].astype(jnp.bfloat16)

    def ship(j):
        target, cd, k, first = message_rows(j)
        mine = pl.ds(pl.multiple_of(row * cap, cap), cap)
        stays = (target == row) & (cd == col)

        @pl.when(stays)
        def _():
            got[k, mine, :] = packed[k, pl.ds(first, cap), :]

        @pl.when(jnp.logical_not(stays))
        def _():
            pltpu.make_async_remote_copy(
                src_ref=packed.at[k, pl.ds(first, cap)], dst_ref=got.at[k, mine],
                send_sem=trade_send.at[k], recv_sem=trade_recv.at[k],
                device_id=(target, cd), device_id_type=MESH,
            ).start()

    def trade_portion(p):
        def one(i, _):
            j = p * share + i
            collect(j)

            @pl.when(j > 0)
            def _():
                ship(j - 1)

            return 0

        lax.fori_loop(0, share, one, 0)

    def opening(p, _):
        trade_portion(p)
        return 0

    lead = splits + min(LEAD, splits)
    lax.fori_loop(0, lead, opening, 0)

    lanes = 128

    def build_pick(a, _):
        first = pl.multiple_of(a * lanes, lanes)
        place = lax.broadcasted_iota(jnp.int32, (points, lanes), 1) + first
        chosen = slot_ref[...] == place
        pick[:, pl.ds(first, lanes)] = jnp.where(chosen, 1.0, 0.0).astype(jnp.bfloat16)
        return 0

    lax.fori_loop(0, n * cap // lanes, build_pick, 0)

    def unit_rows(u):
        return u // splits, pl.ds(pl.multiple_of(lax.rem(u, splits) * rows_unit, rows_unit), rows_unit)

    def unit(p, u):
        k, rows = unit_rows(u)
        return full.at[p, k, rows]

    def send(p, u, sems, target_row):
        ref = unit(p, u)
        return pltpu.make_async_remote_copy(
            src_ref=ref, dst_ref=ref,
            send_sem=sems.at[p], recv_sem=piece_recv.at[p, u],
            device_id=(target_row, col), device_id_type=MESH,
        )

    def own_copy(q, u, src, slot, target_col):
        k, rows = unit_rows(u)
        return pltpu.make_async_remote_copy(
            src_ref=src, dst_ref=own.at[q, k, rows],
            send_sem=own_send.at[slot], recv_sem=own_recv.at[q, u],
            device_id=(row, target_col), device_id_type=MESH,
        )

    def own_unit(q, u):
        k, rows = unit_rows(u)
        return own.at[q, k, rows]

    def place(p):
        oz, same = p // 2, lax.rem(p, 2) == y
        rim = (oz == 0) | (oz == m - 1)
        rises = (z >= oz) & (z + 1 < m)
        falls = (z <= oz) & (z > 0)
        hops = jnp.abs(z - oz) + jnp.where(same, 0, 1)
        return same, rim, rises, falls, z == oz, hops

    def spread(p, u):
        same, rim, rises, falls, level, _ = place(p)
        flat = rim & (lax.rem(u, FLAT) == 0)

        @pl.when((same | flat) & rises)
        def _():
            send(p, u, up_send, row + 2).start()

        @pl.when((same | flat) & falls)
        def _():
            send(p, u, down_send, row - 2).start()

        @pl.when(same & (level | jnp.logical_not(flat)))
        def _():
            send(p, u, pair_send, pair).start()

        s, q = part_of(p)

        @pl.when(is_root & (s == home_s))
        def _():
            for a in range(1, pairs):
                own_copy(q, u, unit(p, u), a, lax.rem(chip + a, pairs) * 2 + core).start()
            own_copy(q, u, unit(p, u), 0, mate).start()

    def trade_done(sems, k):
        for kept in range(2):
            @pl.when(keeps == kept)
            def _():
                part = got.at[k, pl.ds(0, (n - kept) * cap)]
                pltpu.make_async_copy(part, part, sems.at[k]).wait()

    def compact(v):
        k = v // splits

        @pl.when(lax.rem(v, splits) == 0)
        def _():
            trade_done(trade_recv, k)
            dense = lax.dot_general(
                pick[...], got[k], (((1,), (0,)), ((), ())), preferred_element_type=jnp.float32
            )
            full[row, k] = dense.astype(jnp.bfloat16)

    tile = min(TILE, points)
    items = span * (points // tile)

    def multiply(k, i):
        s, a = i // (points // tile), lax.rem(i, points // tile)
        cols = pl.ds(pl.multiple_of(a * tile, tile), tile)
        rows = pl.ds(pl.multiple_of(s * points, points), points)
        total = None
        for q in range(0, c, 2):
            left = jnp.concatenate([full[place_of(s, q + e, col), k] for e in range(2)], axis=1)
            right = jnp.concatenate([own[q + e, k, cols, :] for e in range(2)], axis=1)
            part = lax.dot_general(
                left, right, (((1,), (1,)), ((), ())), preferred_element_type=jnp.float32
            )
            total = part if total is None else total + part

        @pl.when(k == 0)
        def _():
            o_ref[rows, cols] = total

        @pl.when((k > 0) & (k < kv))
        def _():
            o_ref[rows, cols] += total

        @pl.when((k == kv) & (k < chunks - 1))
        def _():
            cond[rows, cols] = total

        @pl.when((k > kv) & (k < chunks - 1))
        def _():
            cond[rows, cols] += total

        @pl.when(k == chunks - 1)
        def _():
            whole = total if chunks - kv == 1 else cond[rows, cols] + total
            o_ref[rows, cols] *= whole

    compact(0)
    settle = HOP * (m + 2) + splits - 1

    def step(t, _):
        @pl.when(t + lead < units)
        def _():
            trade_portion(t + lead)

        @pl.when(t + lead == units)
        def _():
            ship(messages - 1)

        @pl.when(t < units)
        def _():
            spread(row, t)

        def pieces(p, _):
            hops = place(p)[5]
            u = t - HOP * hops

            @pl.when((hops > 0) & (u >= 0) & (u < units))
            def _():
                send(p, u, pair_send, pair).wait_recv()
                spread(p, u)

            return 0

        @pl.when(t + 1 < units)
        def _():
            compact(t + 1)

        lax.fori_loop(0, n, pieces, 0)

        def take_peer(q, _):
            u = t - HOP * (m + 1)

            @pl.when(is_peer & (u >= 0) & (u < units))
            def _():
                copy = own_copy(q, u, own_unit(q, u), 0, mate)
                copy.wait_recv()
                copy.start()

            return 0

        lax.fori_loop(0, c, take_peer, 0)

        def take_far(q, _):
            u = t - HOP * (m + 2)

            @pl.when(is_far & (u >= 0) & (u < units))
            def _():
                own_copy(q, u, own_unit(q, u), 0, mate).wait_recv()

            return 0

        lax.fori_loop(0, c, take_far, 0)

        w = t - settle

        @pl.when((w >= 0) & (w < units))
        def _():
            k, r = w // splits, lax.rem(w, splits)

            @pl.when(is_root & (r == 0))
            def _():
                def keep(q, _):
                    own[q, k] = full[place_of(home_s, q, col), k]
                    return 0

                lax.fori_loop(0, c, keep, 0)

            def some(i, _):
                multiply(k, r * (items // splits) + i)
                return 0

            lax.fori_loop(0, items // splits, some, 0)

        return 0

    lax.fori_loop(0, units + settle, step, 0)

    flats = (units + FLAT - 1) // FLAT

    def sent(sems, p, count):
        part = stage.at[0, pl.ds(0, count * rows_unit // fold)]
        pltpu.make_async_copy(part, part, sems.at[p]).wait()

    def drain(p, _):
        same, rim, rises, falls, level, _ = place(p)
        other = jnp.logical_not(same)
        short = rim & jnp.logical_not(level)
        for goes, sems, count in (
            (same & rises, up_send, units),
            (same & falls, down_send, units),
            (other & rim & rises, up_send, flats),
            (other & rim & falls, down_send, flats),
            (same & jnp.logical_not(short), pair_send, units),
            (same & short, pair_send, units - flats),
        ):
            @pl.when(goes)
            def _():
                sent(sems, p, count)

        return 0

    lax.fori_loop(0, n, drain, 0)

    @pl.when(is_root)
    def _():
        for p in range(pairs):
            pltpu.make_async_copy(own, own, own_send.at[p]).wait()

    @pl.when(is_peer)
    def _():
        pltpu.make_async_copy(own, own, own_send.at[0]).wait()

    def drain_trade(k, _):
        trade_done(trade_send, k)
        return 0

    lax.fori_loop(0, chunks, drain_trade, 0)


def trade_spread_multiply(valence, conduction, source, slots, n, c, cap):
    points = slots.shape[0]
    wv, wc = valence.shape[1], conduction.shape[1]
    cells = valence.shape[0]
    span = n // c
    pairs = c // 2
    g = LANES
    fold = 2 if wv % (2 * g) == 0 and wc % (2 * g) == 0 else 1
    chunks = (wv + wc) // g
    splits = max(points // UNIT_ROWS, 1)
    units = chunks * splits
    dma = pltpu.SemaphoreType.DMA
    return pl.pallas_call(
        functools.partial(gram_kernel, n, c, cap, wv // g, splits, fold),
        out_shape=pltpu.VMEM((span * points, points), jnp.float32),
        in_specs=[
            pl.BlockSpec(memory_space=pl.ANY),
            pl.BlockSpec(memory_space=pl.ANY),
            pl.BlockSpec(memory_space=pltpu.SMEM),
            pl.BlockSpec(memory_space=pltpu.VMEM),
        ],
        out_specs=pl.BlockSpec(memory_space=pltpu.VMEM),
        scratch_shapes=[
            pltpu.VMEM((chunks // fold, cells, fold * g), jnp.bfloat16),
            pltpu.VMEM((cells, fold * g), jnp.float32),
            pltpu.VMEM((cap, fold * g), jnp.float32),
            pltpu.VMEM((chunks, n * cap, g), jnp.bfloat16),
            pltpu.VMEM((chunks, n * cap, g), jnp.bfloat16),
            pltpu.VMEM((points, n * cap), jnp.bfloat16),
            pltpu.VMEM((n, chunks, points, g), jnp.bfloat16),
            pltpu.VMEM((c, chunks, points, g), jnp.bfloat16),
            pltpu.VMEM((span * points, points), jnp.float32),
            dma((chunks // fold,)),
            dma((chunks,)),
            dma((chunks,)),
            dma((n,)),
            dma((n,)),
            dma((n,)),
            dma((n, units)),
            dma((pairs,)),
            dma((c, units)),
        ],
        compiler_params=pltpu.CompilerParams(
            collective_id=0, has_side_effects=True, vmem_limit_bytes=50 * 1024 * 1024
        ),
    )(valence, conduction, source, slots)


def on_device(valence, conduction, point_index):
    n = lax.axis_size("row")
    c = lax.axis_size("col")
    row, col = lax.axis_index("row"), lax.axis_index("col")
    grid_cells = valence.shape[0]
    points = point_index.shape[0] // n
    cap = max(2 * points // n, 2)
    blocks = point_index.reshape(n, points)
    owners = blocks // grid_cells
    offsets = blocks - owners * grid_cells
    onehot = owners[:, None, :] == jnp.arange(n, dtype=jnp.int32)[None, :, None]
    place = jnp.arange(points, dtype=jnp.int32)
    earlier = (place[:, None] < place[None, :]).astype(jnp.bfloat16)
    before = lax.dot_general(
        onehot.astype(jnp.bfloat16), earlier, (((2,), (0,)), ((), ())),
        preferred_element_type=jnp.float32,
    )
    ranks = jnp.sum(jnp.where(onehot, before, 0.0), axis=1).astype(jnp.int32)
    picked = (owners == row)[:, None, :] & (
        ranks[:, None, :] == jnp.arange(cap, dtype=jnp.int32)[None, :, None]
    )
    source_cells = jnp.sum(jnp.where(picked, offsets[:, None, :], 0), axis=2).reshape(n * cap)
    piece = lax.rem(row - 2 * col + 2 * n, n) // c + col * (n // c)
    slots = lax.dynamic_index_in_dim(owners * cap + ranks, piece, 0, keepdims=False)
    slots = jnp.broadcast_to(slots[:, None], (points, 128))
    return trade_spread_multiply(valence, conduction, source_cells, slots, n, c, cap)


def solution(mesh):
    placed = (P("row", "col"), P("row", "col"), P())
    return jax.shard_map(
        on_device, mesh=mesh, in_specs=placed, out_specs=P("col", "row"), check_vma=False
    )
```
